512 devices in a mesh: row: 16 (over x, y), col: 32 (over z, core).
Axes of the slice: x: 4, y: 4, z: 16, core: 2. Of those that a mesh axis runs over, the one named last changes fastest.
Arguments:
- gradient: float32 [5504, 4096], P('col', 'row'), may hold values from -6 to 6
- ginv: float32 [5504, 5504], P('col', 'row'), may hold values from -1 to 3.5, as said below
- ainv: float32 [4096, 4096], P('col', 'row'), may hold values from -1 to 3.5, as said below
Outputs:
- preconditioned: float32 [5504, 4096], P('col', 'row')
The draws below stay inside these ranges and needn't reach their ends.
Inputs may be any that keep to these rules, and one draw needn't show every extreme that they name: ginv is exactly symmetric and positive definite. ainv is exactly symmetric and positive definite.
All inputs are finite; a program needn't handle non-finite values.
Results may differ from the reference program's by a relative error of at most 0.000086.
Values sent between devices are 32-bit elements; how exact they have to be, the bound alone decides.
A program may use at most 64 MiB of HBM per device.

```python
import math
import jax
import jax.numpy as jnp
from jax import lax

D = 4096
FF = 5504


def symmetric_inverse(seed_key, extent):
    first_key, second_key = jax.random.split(seed_key)
    low_end, high_end = (0.6, 2.0)
    diagonal = jnp.exp(jax.random.uniform(first_key, (extent,), jnp.float32, math.log(low_end), math.log(high_end)))
    gaussian = jax.random.normal(second_key, (extent, extent), jnp.float32)
    coupling = (gaussian + gaussian.T) * (0.25 / math.sqrt(2.0 * extent))
    return coupling + jnp.diag(diagonal)


def draw_ginv(key, part):
    return symmetric_inverse(jax.random.fold_in(key, 11), FF)


def draw_ainv(key, part):
    return symmetric_inverse(jax.random.fold_in(key, 23), D)


def steps_of(key, shape, cuts, low, largest):
    loudness = 1.0
    for axis_at, blocks in cuts:
        draws = jax.random.uniform(jax.random.fold_in(jax.random.fold_in(key, 6), axis_at), (blocks,), jnp.float32, low / len(cuts), largest / len(cuts))
        loudness = loudness * jnp.repeat(jnp.exp(draws), shape[axis_at] // blocks).reshape((-1,) + (1,) * (len(shape) - 1 - axis_at))
    return loudness


def bell_draw(key, dims, scale, limit, pieces=(), held_as=jnp.bfloat16):
    array = scale * jax.random.normal(key, dims, jnp.float32)
    if pieces:
        array = array * steps_of(key, dims, pieces, -0.22, 0.18)
    return jnp.clip(array, -limit, limit).astype(held_as)


def setup_inputs(seed: int = 0) -> dict:
    key_of = jax.random.split(jax.random.key(seed), 4)
    return {
        "gradient": bell_draw(key_of[0], (FF, D), 1.0, 6.0, ((0, 32), (1, 16)), jnp.float32),
        "ginv": draw_ginv(jax.random.fold_in(key_of[3], 71), 0),
        "ainv": draw_ainv(jax.random.fold_in(key_of[3], 71), 0),
    }


def reference(gradient, ginv, ainv):
    left = jnp.dot(ginv, gradient, precision=lax.Precision.HIGHEST, preferred_element_type=jnp.float32)
    return jnp.dot(left, ainv, precision=lax.Precision.HIGHEST, preferred_element_type=jnp.float32)
```

```python
import functools
import heapq

import jax
import jax.numpy as jnp
from jax import lax
from jax.experimental import pallas as pl
from jax.experimental.pallas import tpu as pltpu
from jax.sharding import PartitionSpec as P

MESH = pl.DeviceIdType.MESH
F32 = jnp.float32
BF16 = jnp.bfloat16

X = 4
Z = 16
M = 172
MP = 176
HM = MP // 2
N = 256
NA = 128
KV = 344
KP = 384
PIECES = {"A": 2, "T": 2}
PART = {"A": NA, "T": MP}
LIMIT = (8, 7)
UNITS = (0, -1, 1, 2)
GOES_RIGHT = (0, -1)
TURN = {"G": "right", "V": "left"}


def plane_index(u, v):
    return UNITS.index(u) * 4 + UNITS.index(v)


def plan():
    rate = 90e3
    hop, near, turn = 1.9, 1.0, 0.1
    size = {"G": HM * N * 4, "V": HM * KP * 4, "A": NA * N * 4, "T": MP * N * 4}
    free = {}
    heap = []
    order = []
    count = [0]

    def send(now, link, nbytes, event):
        start = max(now, free.get(link, 0.0))
        pace = 500e3 if link == "d" else rate
        free[link] = start + nbytes / pace
        count[0] += 1
        heapq.heappush(heap, (free[link] + (near if link == "d" else hop), count[0], event))

    def axes(h):
        return ("x", "y") if h == 0 else ("y", "x")

    def plane_send(now, q, h, axis, way, event):
        send(now, axis + way, 2 * size[q], event)

    def plane_own(now, q):
        for h in (0, 1):
            first, second = axes(h)
            plane_send(now, q, h, first, "+", (q, h, -1, 0))
            plane_send(now, q, h, first, "-", (q, h, 1, 0))
        for h in (0, 1):
            first, second = axes(h)
            plane_send(now, q, h, second, "+", (q, h, 0, -1))
            plane_send(now, q, h, second, "-", (q, h, 0, 1))

    def ring_own(now, q):
        for k in range(PIECES[q]):
            send(now, "z", size[q] / PIECES[q], (q, 1, 0, k))
            send(now, "d", size[q] / PIECES[q], (q, 0, 1, k))

    def act(now, event):
        q = event[0]
        if q in "GV":
            _, h, u, v = event
            first, second = axes(h)
            if v == 0:
                if u == -1 and TURN[q] == "right":
                    plane_send(now, q, h, first, "+", (q, h, 2, 0))
                if u == 1 and TURN[q] == "left":
                    plane_send(now, q, h, first, "-", (q, h, 2, 0))
                plane_send(now, q, h, second, "+", (q, h, u, -1))
                plane_send(now, q, h, second, "-", (q, h, u, 1))
            if v == -1 and u in GOES_RIGHT:
                plane_send(now, q, h, second, "+", (q, h, u, 2))
            if v == 1 and u not in GOES_RIGHT:
                plane_send(now, q, h, second, "-", (q, h, u, 2))
        else:
            _, s, p, k = event
            if s < LIMIT[p]:
                send(now, "z", size[q] / PIECES[q], (q, s + 1, p, k))
            if s > 0:
                send(now, "d", size[q] / PIECES[q], ("sibling",))

    plane_own(0.0, "G")
    ring_own(0.0, "A")
    left = {"G": 30, "A": 16 * PIECES["A"], "V": 30, "T": 16 * PIECES["T"]}
    early = 8
    pending = []
    while heap:
        now, _, event = heapq.heappop(heap)
        if event[0] == "sibling":
            continue
        order.append((now, event))
        act(now + turn, event)
        q = event[0]
        left[q] -= 1
        if q == "G" and left[q] == early:
            plane_own(now + turn, "V")
            order.append((now, ("begin", "V")))
        if q in "AG" and left["A"] == 0 and left["G"] == 0:
            ring_own(now + 2.0, "T")
            order.append((now, ("begin", "T")))
    return order


def split(x):
    high = x.astype(BF16)
    return high, (x - high.astype(F32)).astype(BF16)


def product(a, b):
    a1, a2 = split(a)
    b1, b2 = split(b)
    dot = functools.partial(jnp.dot, preferred_element_type=F32)
    return dot(a1, b2) + dot(a2, b1) + dot(a1, b1)


def kernel(
    grad_ref, ginv_ref, ainv_ref, out_ref,
    gbuf, vbuf, abuf, tbuf, acc, gstage, vstage, local,
    g_send, g_recv, v_send, v_recv, az_send, az_recv, as_send, as_recv, tz_send, tz_recv, ts_send, ts_recv,
):
    r, c = lax.axis_index("row"), lax.axis_index("col")
    x, y = r // X, lax.rem(r, X)
    z, core = c // 2, lax.rem(c, 2)
    other = 1 - core
    way = 1 - 2 * core

    def at_xy(dx, dy):
        return lax.rem(x + dx + X, X) * X + lax.rem(y + dy + X, X)

    def at_z(d):
        return lax.rem(z + d + Z, Z)

    ahead = (r, at_z(way) * 2 + core)
    behind = (r, at_z(-way) * 2 + core)
    sibling = (r, z * 2 + other)
    side = {
        ("x", 1): (at_xy(1, 0), c),
        ("x", -1): (at_xy(-1, 0), c),
        ("y", 1): (at_xy(0, 1), c),
        ("y", -1): (at_xy(0, -1), c),
    }

    loads = [
        pltpu.make_async_copy(grad_ref, gstage, local.at[0]),
        pltpu.make_async_copy(ginv_ref, vstage, local.at[1]),
        pltpu.make_async_copy(ainv_ref, abuf.at[z, pl.ds(pl.multiple_of(core * NA, NA), NA)], local.at[2]),
    ]
    for load in loads:
        load.start()
    barrier = pltpu.get_barrier_semaphore()
    peers = [ahead, behind, sibling, *side.values()]
    for peer in peers:
        pl.semaphore_signal(barrier, inc=1, device_id=peer, device_id_type=MESH)

    loads[0].wait()
    gbuf[r, 0:M, :] = gstage[...]
    gbuf[r, M:MP, :] = jnp.zeros((MP - M, N), F32)
    loads[1].wait()
    vbuf[r] = jnp.zeros((MP, KP), F32)
    vbuf[r, 0:M, 0:M] = vstage[:, 0:M]
    vbuf[r, 0:M, MP : MP + M] = vstage[:, M:KV]
    acc[...] = jnp.zeros_like(acc)
    loads[2].wait()
    pl.semaphore_wait(barrier, len(peers))

    plane = {"G": (gbuf, g_send, g_recv), "V": (vbuf, v_send, v_recv)}
    ring = {
        "A": (abuf, az_send, az_recv, as_send, as_recv),
        "T": (tbuf, tz_send, tz_recv, ts_send, ts_recv),
    }
    sent = []

    def origin(h, u, v):
        return at_xy(u, v) if h == 0 else at_xy(v, u)

    def plane_copy(q, h, u, v, to, ru, rv):
        buf, send_sem, recv_sem = plane[q]
        piece = buf.at[origin(h, u, v), pl.ds(h * HM, HM)]
        i = h * 16 + plane_index(ru, rv)
        copy = pltpu.make_async_remote_copy(
            piece, piece, send_sem.at[i], recv_sem.at[i], device_id=to, device_id_type=MESH
        )
        copy.start()
        sent.append(copy)

    def plane_wait(q, h, u, v):
        buf, send_sem, recv_sem = plane[q]
        piece = buf.at[origin(h, u, v), pl.ds(h * HM, HM)]
        i = h * 16 + plane_index(u, v)
        pltpu.make_async_remote_copy(
            piece, piece, send_sem.at[i], recv_sem.at[i], device_id=sibling, device_id_type=MESH
        ).wait_recv()

    def axes(h):
        return ("x", "y") if h == 0 else ("y", "x")

    def across(q, h, u):
        second = axes(h)[1]
        plane_copy(q, h, u, 0, side[second, 1], u, -1)
        plane_copy(q, h, u, 0, side[second, -1], u, 1)

    def plane_own(q):
        for h in (0, 1):
            first = axes(h)[0]
            plane_copy(q, h, 0, 0, side[first, 1], -1, 0)
            plane_copy(q, h, 0, 0, side[first, -1], 1, 0)
        for h in (0, 1):
            across(q, h, 0)

    def plane_event(q, h, u, v):
        plane_wait(q, h, u, v)
        first, second = axes(h)
        if v == 0:
            if u == -1 and TURN[q] == "right":
                plane_copy(q, h, u, 0, side[first, 1], 2, 0)
            if u == 1 and TURN[q] == "left":
                plane_copy(q, h, u, 0, side[first, -1], 2, 0)
            across(q, h, u)
        if v == -1 and u in GOES_RIGHT:
            plane_copy(q, h, u, v, side[second, 1], u, 2)
        if v == 1 and u not in GOES_RIGHT:
            plane_copy(q, h, u, v, side[second, -1], u, 2)

    def piece_of(q, owner, part, k):
        rows = PART[q] // PIECES[q]
        start = pl.multiple_of(part * PART[q] + k * rows, 8)
        return ring[q][0].at[owner, pl.ds(start, rows)]

    def index(q, s, p, k):
        return (s * 2 + p) * PIECES[q] + k

    def ring_block(q, s, p, k):
        return piece_of(q, at_z(-way * s), core if p == 0 else other, k)

    def sibling_block(q, s, p, k):
        return piece_of(q, at_z(way * s), other if p == 0 else core, k)

    def forward(q, s, p, k):
        _, zs, zr, _, _ = ring[q]
        piece = ring_block(q, s, p, k)
        i = index(q, s + 1, p, k)
        copy = pltpu.make_async_remote_copy(piece, piece, zs.at[i], zr.at[i], device_id=ahead, device_id_type=MESH)
        copy.start()
        sent.append(copy)

    def hand_over(q, s, p, k):
        _, _, _, ss, sr = ring[q]
        piece = ring_block(q, s, p, k)
        i = index(q, s, p, k)
        copy = pltpu.make_async_remote_copy(piece, piece, ss.at[i], sr.at[i], device_id=sibling, device_id_type=MESH)
        copy.start()
        sent.append(copy)

    def ring_own(q):
        for k in range(PIECES[q]):
            forward(q, 0, 0, k)
            hand_over(q, 0, 0, k)

    def ring_event(q, s, p, k):
        _, zs, zr, ss, sr = ring[q]
        if s == 0:
            wait_sibling(q, 0, 0, k)
        else:
            piece = ring_block(q, s, p, k)
            i = index(q, s, p, k)
            pltpu.make_async_remote_copy(
                piece, piece, zs.at[i], zr.at[i], device_id=sibling, device_id_type=MESH
            ).wait_recv()
        if s < LIMIT[p]:
            forward(q, s, p, k)
        if s > 0:
            hand_over(q, s, p, k)

    def wait_sibling(q, s, p, k):
        _, _, _, ss, sr = ring[q]
        piece = sibling_block(q, s, p, k)
        i = index(q, s, p, k)
        pltpu.make_async_remote_copy(
            piece, piece, ss.at[i], sr.at[i], device_id=sibling, device_id_type=MESH
        ).wait_recv()

    def grad_dot(owner):
        acc[...] += product(gbuf[owner], abuf[owner])

    def ginv_dot(owner):
        acc[...] += product(vbuf[owner][:, 0 : 2 * MP], tbuf[owner])

    dots = {"A": grad_dot, "T": ginv_dot}

    def do_dot(q, e):
        if 0 < e < 8:
            for k in range(PIECES[q]):
                wait_sibling(q, e, 0, k)
                wait_sibling(q, e, 1, k)
        if e == 8:
            for k in range(PIECES[q]):
                wait_sibling(q, 8, 0, k)
        dots[q](at_z(way * e))

    plane_own("G")
    ring_own("A")
    left = {"G": 30, "V": 30}
    ready = []
    seen = {}

    def drain(q, at_most):
        for _ in range(min(at_most, len(ready))):
            do_dot(q, ready.pop(0))

    def note_ring(q, s, p):
        seen[q, s] = seen.get((q, s), 0) + 1
        if s == 8:
            if seen[q, s] == PIECES[q]:
                ready.append(8)
        elif s == 0:
            if seen[q, s] == PIECES[q]:
                ready.append(0)
        elif seen[q, s] == 2 * PIECES[q]:
            ready.extend([-s, s])

    for _, event in plan():
        q = event[0]
        if q == "begin":
            if event[1] == "V":
                plane_own("V")
            else:
                drain("A", len(ready))
                tbuf[z, pl.ds(pl.multiple_of(core * MP, 8), MP), :] = acc[...]
                ring_own("T")
                acc[...] = jnp.zeros_like(acc)
        elif q in "GV":
            plane_event(*event)
            left[q] -= 1
            if q == "G" and left["G"] == 0:
                pass
        else:
            ring_event(*event)
            note_ring(q, event[1], event[2])
            if q == "A" and left["G"] == 0 or q == "T" and left["V"] == 0:
                drain(q, 3)
    drain("T", len(ready))
    out_ref[...] = acc[0:M, :]
    for copy in sent:
        copy.wait_send()


def body(gradient, ginv, ainv):
    na, nt = 18 * PIECES["A"], 18 * PIECES["T"]
    sem = pltpu.SemaphoreType.DMA
    return pl.pallas_call(
        kernel,
        name="precondition",
        out_shape=jax.ShapeDtypeStruct((M, N), F32),
        in_specs=[pl.BlockSpec(memory_space=pl.ANY)] * 3,
        out_specs=pl.BlockSpec(memory_space=pltpu.VMEM),
        scratch_shapes=[
            pltpu.VMEM((X * X, MP, N), F32),
            pltpu.VMEM((X * X, MP, KP), F32),
            pltpu.VMEM((Z, 2 * NA, N), F32),
            pltpu.VMEM((Z, 2 * MP, N), F32),
            pltpu.VMEM((MP, N), F32),
            pltpu.VMEM((M, N), F32),
            pltpu.VMEM((M, KV), F32),
            sem((3,)),
            sem((32,)),
            sem((32,)),
            sem((32,)),
            sem((32,)),
            *[sem((na,))] * 4,
            *[sem((nt,))] * 4,
        ],
        compiler_params=pltpu.CompilerParams(
            collective_id=0, has_side_effects=True, vmem_limit_bytes=60 * 1024 * 1024
        ),
    )(gradient, ginv, ainv)


def solution(mesh):
    return jax.shard_map(
        body,
        mesh=mesh,
        in_specs=(P("col", "row"), P("col", "row"), P("col", "row")),
        out_specs=P("col", "row"),
        check_vma=False,
    )
```
